8 devices in a mesh: dp: 1 (over z), tp: 8 (over y, x, core).
Axes of the slice: x: 2, y: 2, z: 1, core: 2. Of those that a mesh axis runs over, the one named last changes fastest.
Arguments:
- x_norm: bfloat16 [256, 3072], P(('dp', 'tp'))
- w_gate: bfloat16 [3072, 8192], P(None, 'tp')
- w_up: bfloat16 [3072, 8192], P(None, 'tp')
- w_down: bfloat16 [8192, 3072], P('tp')
- u_gate: bfloat16 [256, 8192], P('dp', 'tp')
- u_up: bfloat16 [256, 8192], P('dp', 'tp')
- grad_out: bfloat16 [256, 3072], P(('dp', 'tp'))
Outputs:
- output 1: bfloat16 [256, 3072], P(('dp', 'tp'))
- output 2: float32 [3072, 8192], P('dp', 'tp')
- output 3: float32 [3072, 8192], P('dp', 'tp')
- output 4: float32 [8192, 3072], P(('dp', 'tp'))
All inputs are finite; a program needn't handle non-finite values.
Results may differ from the reference program's by a relative error of at most 0.0116367.
Values are sent between devices in bfloat16 or wider.
A program may use at most 1 GiB of HBM per device.

```python
import jax
import jax.numpy as jnp

TOKENS = 256
HIDDEN = 3072
FFN_DIM = 8192


def setup_inputs(seed: int = 0, part: int = 0) -> dict:
    shared_keys = jax.random.split(jax.random.key(seed + 1), 3)
    own_keys = jax.random.split(jax.random.fold_in(jax.random.key(seed), part), 4)
    x_norm = jax.random.normal(own_keys[0], (TOKENS, HIDDEN), jnp.float32)
    w_gate = jax.random.normal(shared_keys[0], (HIDDEN, FFN_DIM), jnp.float32) * HIDDEN ** -0.5
    w_up = jax.random.normal(shared_keys[1], (HIDDEN, FFN_DIM), jnp.float32) * HIDDEN ** -0.5
    w_down = jax.random.normal(shared_keys[2], (FFN_DIM, HIDDEN), jnp.float32) * FFN_DIM ** -0.5
    u_gate = jax.random.normal(own_keys[1], (TOKENS, FFN_DIM), jnp.float32)
    u_up = jax.random.normal(own_keys[2], (TOKENS, FFN_DIM), jnp.float32)
    grad_out = jax.random.normal(own_keys[3], (TOKENS, HIDDEN), jnp.float32)
    return {
        'x_norm': x_norm.astype(jnp.bfloat16),
        'w_gate': w_gate.astype(jnp.bfloat16),
        'w_up': w_up.astype(jnp.bfloat16),
        'w_down': w_down.astype(jnp.bfloat16),
        'u_gate': u_gate.astype(jnp.bfloat16),
        'u_up': u_up.astype(jnp.bfloat16),
        'grad_out': grad_out.astype(jnp.bfloat16),
    }


def reference(x_norm, w_gate, w_up, w_down, u_gate, u_up, grad_out):
    gate_pre = u_gate.astype(jnp.float32)
    up_pre = u_up.astype(jnp.float32)
    sig_gate = jax.nn.sigmoid(gate_pre)
    gate_act = gate_pre * sig_gate
    z_act = (gate_act * up_pre).astype(jnp.bfloat16)
    grad_down = jnp.dot(z_act.T, grad_out, preferred_element_type=jnp.float32)
    grad_hid = jnp.dot(grad_out, w_down.T, preferred_element_type=jnp.float32)
    grad_up = (grad_hid * gate_act).astype(jnp.bfloat16)
    silu_prime = sig_gate * (1.0 + gate_pre * (1.0 - sig_gate))
    grad_gate = (grad_hid * up_pre * silu_prime).astype(jnp.bfloat16)
    grad_x = (jnp.dot(grad_gate, w_gate.T, preferred_element_type=jnp.float32)
              + jnp.dot(grad_up, w_up.T, preferred_element_type=jnp.float32)).astype(jnp.bfloat16)
    grad_wg = jnp.dot(x_norm.T, grad_gate, preferred_element_type=jnp.float32)
    grad_wu = jnp.dot(x_norm.T, grad_up, preferred_element_type=jnp.float32)
    return (grad_x, grad_wg, grad_wu, grad_down)
```

```python
import jax
import jax.numpy as jnp
from jax import lax
from jax.experimental import pallas as pl
from jax.experimental.pallas import tpu as pltpu
from jax.sharding import PartitionSpec as P

CONTRACT_ROWS = (((0,), (0,)), ((), ()))
CONTRACT_COLS = (((1,), (1,)), ((), ()))
F32 = jnp.float32
BF16 = jnp.bfloat16
MIB = 2 ** 20

ROWS = 32
CHUNKS = 4
DX_CHUNK = 512
FROM_X, FROM_Y, FROM_D, FROM_P, PART_X, PART_Y, PART_D = range(7)
TO_X, TO_Y, TO_P, RELAY, FWD_X, FWD_Y, FWD_D = range(7)


def gather_kernel(x_in, dy_in, wg_in, wu_in, wd_in, ug_in, uu_in,
                  x_out, dy_out, z_out, dug_out, duu_out, own_out, px_out, py_out, pd_out,
                  x_all, dy_all, wg, wu, wd, ug, uu, act, slope, z, dug, duu, grad, part, mine, give, take, piece,
                  send_sem, recv_sem, give_sem, take_sem, load_sem, wd_sem, wg_sem, wu_sem, out_sem):
    me = lax.axis_index('tp')
    core = lax.rem(me, 2)
    chip = lax.div(me, 2)
    other = me + 1 - 2 * core
    step_x = 2 - 4 * lax.rem(chip, 2)
    step_y = 4 - 8 * lax.div(chip, 2)
    near_x, near_y, far = me + step_x, me + step_y, me + step_x + step_y
    p_x, p_y, p_d = other + step_x, other + step_y, other + step_x + step_y
    hidden = x_all.shape[1]
    width = hidden // CHUNKS
    n_dx = hidden // DX_CHUNK

    def block(buf, owner, c):
        return buf.at[pl.ds(pl.multiple_of(owner * ROWS, ROWS), ROWS), pl.ds(c * width, width)]

    def rows(buf, owner):
        return buf.at[pl.ds(pl.multiple_of(owner * ROWS, ROWS), ROWS), :]

    own_dy = pltpu.make_async_copy(dy_in, rows(dy_all, me), load_sem.at[0])
    own_x = pltpu.make_async_copy(x_in, rows(x_all, me), load_sem.at[1])
    get_ug = pltpu.make_async_copy(ug_in, ug, load_sem.at[2])
    get_uu = pltpu.make_async_copy(uu_in, uu, load_sem.at[3])
    own_dy.start()
    own_x.start()
    get_ug.start()
    get_uu.start()

    def wd_load(c):
        s = pl.ds(c * width, width)
        return pltpu.make_async_copy(wd_in.at[:, s], wd.at[:, s], wd_sem.at[c])

    def w_loads(h):
        s = pl.ds(h * DX_CHUNK, DX_CHUNK)
        return (pltpu.make_async_copy(wg_in.at[s, :], wg.at[s, :], wg_sem.at[h]),
                pltpu.make_async_copy(wu_in.at[s, :], wu.at[s, :], wu_sem.at[h]))

    for c in range(CHUNKS):
        wd_load(c).start()
    for h in range(n_dx):
        for load in w_loads(h):
            load.start()

    barrier = pltpu.get_barrier_semaphore()
    for peer in (other, near_x, near_y):
        pl.semaphore_signal(barrier, inc=1, device_id={'tp': peer}, device_id_type=pl.DeviceIdType.MESH)
    pl.semaphore_wait(barrier, 3)

    bufs = (dy_all, x_all)

    def copy(a, owner, c, to, send_kind, recv_kind):
        ref = block(bufs[a], owner, c)
        return pltpu.make_async_remote_copy(
            src_ref=ref, dst_ref=ref, send_sem=send_sem.at[a, send_kind, c], recv_sem=recv_sem.at[a, recv_kind, c],
            device_id={'tp': to}, device_id_type=pl.DeviceIdType.MESH)

    started = []

    def send(*args):
        cp = copy(*args)
        cp.start()
        started.append(cp)

    def arrived(a, owner, c, recv_kind):
        copy(a, owner, c, other, TO_P, recv_kind).wait_recv()

    half = CHUNKS // 2
    first = list(range(half))
    last = list(range(half, CHUNKS))

    def send_own(a):
        for c1, c2 in zip(first + last, last + first):
            send(a, me, c1, near_x, TO_X, FROM_X)
            send(a, me, c2, near_y, TO_Y, FROM_Y)
        for c in first + last:
            send(a, me, c, other, TO_P, FROM_P)

    def relay_step(a, i):
        c1, c2 = first[i], last[i]
        arrived(a, near_x, c1, FROM_X)
        send(a, near_x, c1, near_y, RELAY, FROM_D)
        send(a, near_x, c1, other, FWD_X, PART_X)
        arrived(a, near_y, c2, FROM_Y)
        send(a, near_y, c2, near_x, RELAY, FROM_D)
        send(a, near_y, c2, other, FWD_Y, PART_Y)

    def rest_step(a, i):
        c1, c2 = last[i], first[i]
        arrived(a, near_x, c1, FROM_X)
        send(a, near_x, c1, other, FWD_X, PART_X)
        arrived(a, near_y, c2, FROM_Y)
        send(a, near_y, c2, other, FWD_Y, PART_Y)

    def far_step(a, i):
        for c in (first[i], last[i]):
            arrived(a, far, c, FROM_D)
            send(a, far, c, other, FWD_D, PART_D)

    def partner_step(a, c):
        arrived(a, other, c, FROM_P)
        arrived(a, p_x, c, PART_X)
        arrived(a, p_y, c, PART_Y)
        arrived(a, p_d, c, PART_D)

    own_dy.wait()
    send_own(0)

    get_ug.wait()
    get_uu.wait()
    n_e = 8
    for r in range(n_e):
        s = pl.ds(r * (256 // n_e), 256 // n_e)
        gate = ug[s, :].astype(F32)
        sig = jax.nn.sigmoid(gate)
        a = gate * sig
        act[s, :] = a
        slope[s, :] = sig * (1.0 + gate * (1.0 - sig))
        z[s, :] = (a * uu[s, :].astype(F32)).astype(BF16)
    outs = [pltpu.make_async_copy(z, z_out, out_sem.at[0])]
    outs[-1].start()
    own_x.wait()

    for i in range(half):
        relay_step(0, i)
    send_own(1)
    for i in range(half):
        rest_step(0, i)

    fresh = True
    for i in range(half):
        far_step(0, i)
    for i in range(half):
        for c in (first[i], last[i]):
            partner_step(0, c)
            wd_load(c).wait()
            s = pl.ds(c * width, width)
            term = lax.dot_general(dy_all[:, s], wd[:, s], CONTRACT_COLS, preferred_element_type=F32)
            if fresh:
                grad[...] = term
            else:
                grad[...] += term
            fresh = False
    outs.append(pltpu.make_async_copy(dy_all, dy_out, out_sem.at[1]))
    outs[-1].start()

    for i in range(half):
        relay_step(1, i)
    for r in range(n_e):
        s = pl.ds(r * (256 // n_e), 256 // n_e)
        g = grad[s, :]
        duu[s, :] = (g * act[s, :]).astype(BF16)
        dug[s, :] = (g * uu[s, :].astype(F32) * slope[s, :]).astype(BF16)
    outs.append(pltpu.make_async_copy(dug, dug_out, out_sem.at[2]))
    outs[-1].start()
    outs.append(pltpu.make_async_copy(duu, duu_out, out_sem.at[3]))
    outs[-1].start()

    def give_copy(h):
        s = pl.ds(h * DX_CHUNK, DX_CHUNK)
        return pltpu.make_async_remote_copy(
            src_ref=give.at[:, s], dst_ref=take.at[:, s], send_sem=give_sem.at[h], recv_sem=take_sem.at[h],
            device_id={'tp': other}, device_id_type=pl.DeviceIdType.MESH)

    def combine(h):
        s = pl.ds(h * DX_CHUNK, DX_CHUNK)
        give_copy(h).wait_recv()
        piece[:, s] = (mine[:, s] + take[:, s].astype(F32)).astype(BF16)

    x_work = {1: lambda: rest_step(1, 0), 3: lambda: rest_step(1, 1), 4: lambda: far_step(1, 0)}
    for h in range(n_dx):
        for load in w_loads(h):
            load.wait()
        s = pl.ds(h * DX_CHUNK, DX_CHUNK)
        part[...] = (lax.dot_general(dug[...], wg[s, :], CONTRACT_COLS, preferred_element_type=F32)
                     + lax.dot_general(duu[...], wu[s, :], CONTRACT_COLS, preferred_element_type=F32))
        for j in range(4):
            d = pl.ds(j * ROWS, ROWS)
            give[d, s] = part[pl.ds(pl.multiple_of(j * 2 * ROWS + ROWS * (1 - core), ROWS), ROWS), :].astype(BF16)
            mine[d, s] = part[pl.ds(pl.multiple_of(j * 2 * ROWS + ROWS * core, ROWS), ROWS), :]
        give_copy(h).start()
        if h >= 2:
            combine(h - 2)
        if h in x_work:
            x_work[h]()
    far_step(1, 1)
    for h in range(n_dx - 2, n_dx):
        combine(h)
    for k, (ref, flip) in enumerate(((own_out, 0), (px_out, 1), (py_out, 2), (pd_out, 3))):
        fx, fy = flip % 2, flip // 2
        cx, cy = lax.rem(chip, 2), lax.div(chip, 2)
        to_chip = (cx + fx * (1 - 2 * cx)) + 2 * (cy + fy * (1 - 2 * cy))
        outs.append(pltpu.make_async_copy(
            piece.at[pl.ds(pl.multiple_of(to_chip * ROWS, ROWS), ROWS), :], ref, out_sem.at[4 + k]))
        outs[-1].start()
    for c in range(CHUNKS):
        partner_step(1, c)
    outs.append(pltpu.make_async_copy(x_all, x_out, out_sem.at[8]))
    outs[-1].start()
    for cp in started:
        cp.wait_send()
    for h in range(n_dx):
        give_copy(h).wait_send()
    for cp in outs:
        cp.wait()


def gather_call(x, dy, wg, wu, wd, ug, uu):
    hidden, f = wg.shape
    tokens = ug.shape[0]
    n_dx = hidden // DX_CHUNK
    any_spec = pl.BlockSpec(memory_space=pl.ANY)
    shape = jax.ShapeDtypeStruct
    full, act, row = shape((tokens, hidden), BF16), shape((tokens, f), BF16), shape((ROWS, hidden), BF16)
    dma = pltpu.SemaphoreType.DMA
    vmem = pltpu.VMEM
    return pl.pallas_call(
        gather_kernel,
        out_shape=(full, full, act, act, act, row, row, row, row),
        in_specs=[any_spec] * 7,
        out_specs=[any_spec] * 9,
        scratch_shapes=[
            vmem((tokens, hidden), BF16), vmem((tokens, hidden), BF16),
            vmem((hidden, f), BF16), vmem((hidden, f), BF16), vmem((f, hidden), BF16),
            vmem((tokens, f), BF16), vmem((tokens, f), BF16),
            vmem((tokens, f), F32), vmem((tokens, f), F32),
            vmem((tokens, f), BF16), vmem((tokens, f), BF16), vmem((tokens, f), BF16),
            vmem((tokens, f), F32), vmem((tokens, DX_CHUNK), F32),
            vmem((4 * ROWS, hidden), F32), vmem((4 * ROWS, hidden), BF16),
            vmem((4 * ROWS, hidden), BF16), vmem((4 * ROWS, hidden), BF16),
            dma((2, 7, CHUNKS)), dma((2, 7, CHUNKS)), dma((n_dx,)), dma((n_dx,)),
            dma((4,)), dma((CHUNKS,)), dma((n_dx,)), dma((n_dx,)), dma((9,)),
        ],
        compiler_params=pltpu.CompilerParams(collective_id=0, has_side_effects=True, vmem_limit_bytes=48 * MIB),
        cost_estimate=pl.CostEstimate(flops=6 * tokens * hidden * f, bytes_accessed=24 * MIB, transcendentals=0),
        name='gather_and_input_grad',
    )(x, dy, wg, wu, wd, ug, uu)


def weight_kernel(x, dy, z, dug, duu, dwg, dwu, dwd):
    xb = x[...]
    dwg[...] = lax.dot_general(xb, dug[...], CONTRACT_ROWS, preferred_element_type=F32)
    dwu[...] = lax.dot_general(xb, duu[...], CONTRACT_ROWS, preferred_element_type=F32)
    dwd[...] = lax.dot_general(z[...], dy[...], CONTRACT_ROWS, preferred_element_type=F32)


def weight_call(x, dy, z, dug, duu, steps=12):
    tokens, hidden = x.shape
    f = z.shape[1]
    h = hidden // steps
    cols = pl.BlockSpec((tokens, h), lambda i: (0, i))
    whole = pl.BlockSpec((tokens, f), lambda i: (0, 0))
    tall = pl.BlockSpec((h, f), lambda i: (i, 0))
    wide = pl.BlockSpec((f, h), lambda i: (0, i))
    return pl.pallas_call(
        weight_kernel,
        grid=(steps,),
        in_specs=[cols, cols, whole, whole, whole],
        out_specs=[tall, tall, wide],
        out_shape=(jax.ShapeDtypeStruct((hidden, f), F32), jax.ShapeDtypeStruct((hidden, f), F32),
                   jax.ShapeDtypeStruct((f, hidden), F32)),
        compiler_params=pltpu.CompilerParams(vmem_limit_bytes=40 * MIB),
        cost_estimate=pl.CostEstimate(flops=6 * tokens * hidden * f, bytes_accessed=42 * MIB, transcendentals=0),
        name='weight_grads',
    )(x, dy, z, dug, duu)


def solution(mesh):
    n = mesh.shape['tp']

    def local_backward(x, wg, wu, wd, ug, uu, dy):
        x_all, dy_all, z, dug, duu, own, px, py, pd = gather_call(x, dy, wg, wu, wd, ug, uu)

        def swap(v, k):
            return lax.ppermute(v, 'tp', [(i, i ^ k) for i in range(n)])

        rx, ry, rd = swap(px, 2), swap(py, 4), swap(pd, 6)
        dwg, dwu, dwd = weight_call(x_all, dy_all, z, dug, duu)
        dx = (own.astype(F32) + rx.astype(F32) + ry.astype(F32) + rd.astype(F32)).astype(BF16)
        return dx, dwg, dwu, dwd

    tok_spec = P(('dp', 'tp'), None)
    col_spec = P(None, 'tp')
    act_spec = P('dp', 'tp')
    return jax.shard_map(local_backward, mesh=mesh,
                         in_specs=(tok_spec, col_spec, col_spec, P('tp', None), act_spec, act_spec, tok_spec),
                         out_specs=(tok_spec, act_spec, act_spec, tok_spec),
                         check_vma=False)
```

```python
import jax
import jax.numpy as jnp
from jax import lax
from jax.experimental import pallas as pl
from jax.experimental.pallas import tpu as pltpu
from jax.sharding import PartitionSpec as P

CONTRACT_ROWS = (((0,), (0,)), ((), ()))
CONTRACT_COLS = (((1,), (1,)), ((), ()))
F32 = jnp.float32
BF16 = jnp.bfloat16
MIB = 2 ** 20

ROWS = 32
CHUNKS = 4
DX_CHUNK = 512
FROM_X, FROM_Y, FROM_D, FROM_P, PART_X, PART_Y, PART_D = range(7)
TO_X, TO_Y, TO_P, RELAY, FWD_X, FWD_Y, FWD_D = range(7)


def gather_kernel(x_in, dy_in, wg_in, wu_in, wd_in, ug_in, uu_in,
                  x_all, dy_all, z, dug, duu, own_out, px_out, py_out, pd_out,
                  wg, wu, wd, ug, uu, act, slope, grad, part, mine, give, take,
                  send_sem, recv_sem, give_sem, take_sem, load_sem, wd_sem, wg_sem, wu_sem):
    me = lax.axis_index('tp')
    core = lax.rem(me, 2)
    chip = lax.div(me, 2)
    other = me + 1 - 2 * core
    step_x = 2 - 4 * lax.rem(chip, 2)
    step_y = 4 - 8 * lax.div(chip, 2)
    near_x, near_y, far = me + step_x, me + step_y, me + step_x + step_y
    p_x, p_y, p_d = other + step_x, other + step_y, other + step_x + step_y
    hidden = x_all.shape[1]
    width = hidden // CHUNKS
    n_dx = hidden // DX_CHUNK

    def block(buf, owner, c):
        return buf.at[pl.ds(pl.multiple_of(owner * ROWS, ROWS), ROWS), pl.ds(c * width, width)]

    def rows(buf, owner):
        return buf.at[pl.ds(pl.multiple_of(owner * ROWS, ROWS), ROWS), :]

    own_dy = pltpu.make_async_copy(dy_in, rows(dy_all, me), load_sem.at[0])
    own_x = pltpu.make_async_copy(x_in, rows(x_all, me), load_sem.at[1])
    get_ug = pltpu.make_async_copy(ug_in, ug, load_sem.at[2])
    get_uu = pltpu.make_async_copy(uu_in, uu, load_sem.at[3])
    own_dy.start()
    own_x.start()
    get_ug.start()
    get_uu.start()

    def wd_load(c):
        s = pl.ds(c * width, width)
        return pltpu.make_async_copy(wd_in.at[:, s], wd.at[:, s], wd_sem.at[c])

    def w_loads(h):
        s = pl.ds(h * DX_CHUNK, DX_CHUNK)
        return (pltpu.make_async_copy(wg_in.at[s, :], wg.at[s, :], wg_sem.at[h]),
                pltpu.make_async_copy(wu_in.at[s, :], wu.at[s, :], wu_sem.at[h]))

    for c in range(CHUNKS):
        wd_load(c).start()
    for h in range(n_dx):
        for load in w_loads(h):
            load.start()

    barrier = pltpu.get_barrier_semaphore()
    for peer in (other, near_x, near_y):
        pl.semaphore_signal(barrier, inc=1, device_id={'tp': peer}, device_id_type=pl.DeviceIdType.MESH)
    pl.semaphore_wait(barrier, 3)

    bufs = (dy_all, x_all)

    def copy(a, owner, c, to, send_kind, recv_kind):
        ref = block(bufs[a], owner, c)
        return pltpu.make_async_remote_copy(
            src_ref=ref, dst_ref=ref, send_sem=send_sem.at[a, send_kind, c], recv_sem=recv_sem.at[a, recv_kind, c],
            device_id={'tp': to}, device_id_type=pl.DeviceIdType.MESH)

    started = []

    def send(*args):
        cp = copy(*args)
        cp.start()
        started.append(cp)

    def arrived(a, owner, c, recv_kind):
        copy(a, owner, c, other, TO_P, recv_kind).wait_recv()

    half = CHUNKS // 2
    first = list(range(half))
    last = list(range(half, CHUNKS))

    def send_own(a):
        for c1, c2 in zip(first + last, last + first):
            send(a, me, c1, near_x, TO_X, FROM_X)
            send(a, me, c2, near_y, TO_Y, FROM_Y)
        for c in first + last:
            send(a, me, c, other, TO_P, FROM_P)

    def relay_step(a, i):
        c1, c2 = first[i], last[i]
        arrived(a, near_x, c1, FROM_X)
        send(a, near_x, c1, near_y, RELAY, FROM_D)
        send(a, near_x, c1, other, FWD_X, PART_X)
        arrived(a, near_y, c2, FROM_Y)
        send(a, near_y, c2, near_x, RELAY, FROM_D)
        send(a, near_y, c2, other, FWD_Y, PART_Y)

    def rest_step(a, i):
        c1, c2 = last[i], first[i]
        arrived(a, near_x, c1, FROM_X)
        send(a, near_x, c1, other, FWD_X, PART_X)
        arrived(a, near_y, c2, FROM_Y)
        send(a, near_y, c2, other, FWD_Y, PART_Y)

    def far_step(a, i):
        for c in (first[i], last[i]):
            arrived(a, far, c, FROM_D)
            send(a, far, c, other, FWD_D, PART_D)

    def partner_step(a, c):
        arrived(a, other, c, FROM_P)
        arrived(a, p_x, c, PART_X)
        arrived(a, p_y, c, PART_Y)
        arrived(a, p_d, c, PART_D)

    own_dy.wait()
    send_own(0)

    get_ug.wait()
    get_uu.wait()
    n_e = 8
    for r in range(n_e):
        s = pl.ds(r * (256 // n_e), 256 // n_e)
        gate = ug[s, :].astype(F32)
        sig = jax.nn.sigmoid(gate)
        a = gate * sig
        act[s, :] = a
        slope[s, :] = sig * (1.0 + gate * (1.0 - sig))
        z[s, :] = (a * uu[s, :].astype(F32)).astype(BF16)
    own_x.wait()

    for i in range(half):
        relay_step(0, i)
    send_own(1)
    for i in range(half):
        rest_step(0, i)

    fresh = True
    for i in range(half):
        far_step(0, i)
    for i in range(half):
        for c in (first[i], last[i]):
            partner_step(0, c)
            wd_load(c).wait()
            s = pl.ds(c * width, width)
            term = lax.dot_general(dy_all[:, s], wd[:, s], CONTRACT_COLS, preferred_element_type=F32)
            if fresh:
                grad[...] = term
            else:
                grad[...] += term
            fresh = False

    for i in range(half):
        relay_step(1, i)
    for r in range(n_e):
        s = pl.ds(r * (256 // n_e), 256 // n_e)
        g = grad[s, :]
        duu[s, :] = (g * act[s, :]).astype(BF16)
        dug[s, :] = (g * uu[s, :].astype(F32) * slope[s, :]).astype(BF16)

    def give_copy(h):
        s = pl.ds(h * DX_CHUNK, DX_CHUNK)
        return pltpu.make_async_remote_copy(
            src_ref=give.at[:, s], dst_ref=take.at[:, s], send_sem=give_sem.at[h], recv_sem=take_sem.at[h],
            device_id={'tp': other}, device_id_type=pl.DeviceIdType.MESH)

    def combine(h):
        s = pl.ds(h * DX_CHUNK, DX_CHUNK)
        give_copy(h).wait_recv()
        for ref, to_chip in ((own_out, chip), (px_out, lax.div(near_x, 2)), (py_out, lax.div(near_y, 2)),
                             (pd_out, lax.div(far, 2))):
            d = pl.ds(pl.multiple_of(to_chip * ROWS, ROWS), ROWS)
            ref[:, s] = (mine[d, s] + take[d, s].astype(F32)).astype(BF16)

    x_work = {1: lambda: rest_step(1, 0), 3: lambda: rest_step(1, 1), 4: lambda: far_step(1, 0)}
    for h in range(n_dx):
        for load in w_loads(h):
            load.wait()
        s = pl.ds(h * DX_CHUNK, DX_CHUNK)
        part[...] = (lax.dot_general(dug[...], wg[s, :], CONTRACT_COLS, preferred_element_type=F32)
                     + lax.dot_general(duu[...], wu[s, :], CONTRACT_COLS, preferred_element_type=F32))
        for j in range(4):
            d = pl.ds(j * ROWS, ROWS)
            give[d, s] = part[pl.ds(pl.multiple_of(j * 2 * ROWS + ROWS * (1 - core), ROWS), ROWS), :].astype(BF16)
            mine[d, s] = part[pl.ds(pl.multiple_of(j * 2 * ROWS + ROWS * core, ROWS), ROWS), :]
        give_copy(h).start()
        if h >= 2:
            combine(h - 2)
        if h in x_work:
            x_work[h]()
    far_step(1, 1)
    for h in range(n_dx - 2, n_dx):
        combine(h)
    for c in range(CHUNKS):
        partner_step(1, c)
    for cp in started:
        cp.wait_send()
    for h in range(n_dx):
        give_copy(h).wait_send()


def gather_call(x, dy, wg, wu, wd, ug, uu):
    hidden, f = wg.shape
    tokens = ug.shape[0]
    n_dx = hidden // DX_CHUNK
    any_spec = pl.BlockSpec(memory_space=pl.ANY)
    x, dy, wg, wu, wd, ug, uu = [pltpu.with_memory_space_constraint(v, pltpu.HBM) for v in (x, dy, wg, wu, wd, ug, uu)]
    vmem = pltpu.VMEM
    full, act, row = vmem((tokens, hidden), BF16), vmem((tokens, f), BF16), vmem((ROWS, hidden), BF16)
    dma = pltpu.SemaphoreType.DMA
    return pl.pallas_call(
        gather_kernel,
        out_shape=(full, full, act, act, act, row, row, row, row),
        in_specs=[any_spec] * 7,
        out_specs=[pl.BlockSpec(memory_space=vmem)] * 9,
        scratch_shapes=[
            vmem((hidden, f), BF16), vmem((hidden, f), BF16), vmem((f, hidden), BF16),
            vmem((tokens, f), BF16), vmem((tokens, f), BF16),
            vmem((tokens, f), F32), vmem((tokens, f), F32),
            vmem((tokens, f), F32), vmem((tokens, DX_CHUNK), F32),
            vmem((4 * ROWS, hidden), F32), vmem((4 * ROWS, hidden), BF16),
            vmem((4 * ROWS, hidden), BF16),
            dma((2, 7, CHUNKS)), dma((2, 7, CHUNKS)), dma((n_dx,)), dma((n_dx,)),
            dma((4,)), dma((CHUNKS,)), dma((n_dx,)), dma((n_dx,)),
        ],
        compiler_params=pltpu.CompilerParams(collective_id=0, has_side_effects=True, vmem_limit_bytes=48 * MIB),
        cost_estimate=pl.CostEstimate(flops=6 * tokens * hidden * f, bytes_accessed=24 * MIB, transcendentals=0),
        name='gather_and_input_grad',
    )(x, dy, wg, wu, wd, ug, uu)


def weight_kernel(x, dy, z, dug, duu, dwg, dwu, dwd):
    xb = x[...]
    dwg[...] = lax.dot_general(xb, dug[...], CONTRACT_ROWS, preferred_element_type=F32)
    dwu[...] = lax.dot_general(xb, duu[...], CONTRACT_ROWS, preferred_element_type=F32)
    dwd[...] = lax.dot_general(z[...], dy[...], CONTRACT_ROWS, preferred_element_type=F32)


def weight_call(x, dy, z, dug, duu, steps=12):
    tokens, hidden = x.shape
    f = z.shape[1]
    h = hidden // steps
    cols = pl.BlockSpec((tokens, h), lambda i: (0, i))
    whole = pl.BlockSpec((tokens, f), lambda i: (0, 0))
    tall = pl.BlockSpec((h, f), lambda i: (i, 0))
    wide = pl.BlockSpec((f, h), lambda i: (0, i))
    return pl.pallas_call(
        weight_kernel,
        grid=(steps,),
        in_specs=[cols, cols, whole, whole, whole],
        out_specs=[tall, tall, wide],
        out_shape=(jax.ShapeDtypeStruct((hidden, f), F32), jax.ShapeDtypeStruct((hidden, f), F32),
                   jax.ShapeDtypeStruct((f, hidden), F32)),
        compiler_params=pltpu.CompilerParams(vmem_limit_bytes=40 * MIB),
        cost_estimate=pl.CostEstimate(flops=6 * tokens * hidden * f, bytes_accessed=42 * MIB, transcendentals=0),
        name='weight_grads',
    )(x, dy, z, dug, duu)


def solution(mesh):
    n = mesh.shape['tp']

    def local_backward(x, wg, wu, wd, ug, uu, dy):
        x_all, dy_all, z, dug, duu, own, px, py, pd = gather_call(x, dy, wg, wu, wd, ug, uu)

        def swap(v, k):
            return lax.ppermute(v, 'tp', [(i, i ^ k) for i in range(n)])

        rx, ry, rd = swap(px, 2), swap(py, 4), swap(pd, 6)
        dwg, dwu, dwd = weight_call(x_all, dy_all, z, dug, duu)
        dx = (own.astype(F32) + rx.astype(F32) + ry.astype(F32) + rd.astype(F32)).astype(BF16)
        return dx, dwg, dwu, dwd

    tok_spec = P(('dp', 'tp'), None)
    col_spec = P(None, 'tp')
    act_spec = P('dp', 'tp')
    return jax.shard_map(local_backward, mesh=mesh,
                         in_specs=(tok_spec, col_spec, col_spec, P('tp', None), act_spec, act_spec, tok_spec),
                         out_specs=(tok_spec, act_spec, act_spec, tok_spec),
                         check_vma=False)
```

```python
import jax
import jax.numpy as jnp
from jax import lax
from jax.experimental import pallas as pl
from jax.experimental.pallas import tpu as pltpu
from jax.sharding import PartitionSpec as P

CONTRACT_ROWS = (((0,), (0,)), ((), ()))
CONTRACT_COLS = (((1,), (1,)), ((), ()))
F32 = jnp.float32
BF16 = jnp.bfloat16
MIB = 2 ** 20

ROWS = 32
DY_CHUNKS = 4
X_CHUNKS = 2
DX_CHUNK = 1024
E_BLOCKS = 8
MESH = pl.DeviceIdType.MESH


def gather_kernel(x_in, dy_in, wg_in, wu_in, wd_in, ug_in, uu_in,
                  x_all, dy_all, z, dug, duu, own_out, px_out, py_out, pd_out,
                  wgu, wd, ugu, act, slope, grad, part, mine, give, take,
                  dy_x, dy_y, dy_d, dy_p, x_x, x_y, x_d, x_p, sent, give_sem, take_sem, own_sem, load_sem):
    me = lax.axis_index('tp')
    core = lax.rem(me, 2)
    chip = lax.div(me, 2)
    other = me + 1 - 2 * core
    step_x = 2 - 4 * lax.rem(chip, 2)
    step_y = 4 - 8 * lax.div(chip, 2)
    near_x, near_y, far = me + step_x, me + step_y, me + step_x + step_y
    tokens, hidden = x_all.shape
    f = dug.shape[1]
    n_dx = hidden // DX_CHUNK

    def rows(buf, owner):
        return buf.at[pl.ds(pl.multiple_of(owner * ROWS, ROWS), ROWS), :]

    own_dy = pltpu.make_async_copy(dy_in, rows(dy_all, me), own_sem.at[0])
    own_x = pltpu.make_async_copy(x_in, rows(x_all, me), own_sem.at[1])
    own_dy.start()
    own_x.start()

    barrier = pltpu.get_barrier_semaphore()
    for peer in (other, near_x, near_y):
        pl.semaphore_signal(barrier, inc=1, device_id={'tp': peer}, device_id_type=MESH)
    pl.semaphore_wait(barrier, 3)

    def block(a, owner, c):
        buf, n = ((dy_all, DY_CHUNKS), (x_all, X_CHUNKS))[a]
        w = hidden // n
        return buf.at[pl.ds(pl.multiple_of(owner * ROWS, ROWS), ROWS), pl.ds(c * w, w)]

    recv = ((dy_x, dy_y, dy_d, dy_p), (x_x, x_y, x_d, x_p))

    def copy(a, owner, c, to, kind):
        ref = block(a, owner, c)
        index = 0 if (a == 1 and kind == 3) else c
        return pltpu.make_async_remote_copy(
            src_ref=ref, dst_ref=ref, send_sem=sent.at[a], recv_sem=recv[a][kind].at[index],
            device_id={'tp': to}, device_id_type=MESH)

    def halves(a):
        n = (DY_CHUNKS, X_CHUNKS)[a]
        return list(range(n // 2)), list(range(n // 2, n))

    def send_own(a):
        lo, hi = halves(a)
        for c1, c2 in zip(lo + hi, hi + lo):
            copy(a, me, c1, near_x, 0).start()
            copy(a, me, c2, near_y, 1).start()
        for c in lo + hi:
            copy(a, me, c, other, 3).start()

    def relay_step(a, i):
        lo, hi = halves(a)
        copy(a, near_x, lo[i], other, 0).wait_recv()
        copy(a, near_x, lo[i], near_y, 2).start()
        copy(a, near_x, lo[i], other, 3).start()
        copy(a, near_y, hi[i], other, 1).wait_recv()
        copy(a, near_y, hi[i], near_x, 2).start()
        copy(a, near_y, hi[i], other, 3).start()

    def rest_step(a, i):
        lo, hi = halves(a)
        copy(a, near_x, hi[i], other, 0).wait_recv()
        copy(a, near_x, hi[i], other, 3).start()
        copy(a, near_y, lo[i], other, 1).wait_recv()
        copy(a, near_y, lo[i], other, 3).start()

    def far_step(a, i):
        for part_of in halves(a):
            copy(a, far, part_of[i], other, 2).wait_recv()
            copy(a, far, part_of[i], other, 3).start()

    def elementwise(blocks):
        n = tokens // E_BLOCKS
        for r in blocks:
            s = pl.ds(r * n, n)
            gate = ugu[s, :].astype(F32)
            sig = jax.nn.sigmoid(gate)
            a = gate * sig
            act[s, :] = a
            slope[s, :] = sig * (1.0 + gate * (1.0 - sig))
            z[s, :] = (a * ugu[pl.ds(tokens + r * n, n), :].astype(F32)).astype(BF16)

    get_ug = pltpu.make_async_copy(ug_in, ugu.at[pl.ds(0, tokens), :], load_sem.at[0])
    get_uu = pltpu.make_async_copy(uu_in, ugu.at[pl.ds(tokens, tokens), :], load_sem.at[0])
    get_wd = pltpu.make_async_copy(wd_in, wd, load_sem.at[1])
    get_wg = pltpu.make_async_copy(wg_in, wgu.at[pl.ds(0, hidden), :], load_sem.at[2])
    get_wu = pltpu.make_async_copy(wu_in, wgu.at[pl.ds(hidden, hidden), :], load_sem.at[2])
    own_dy.wait()
    send_own(0)
    for load in (get_ug, get_uu, get_wd, get_wg, get_wu):
        load.start()
    pltpu.make_async_copy(ugu, ugu, load_sem.at[0]).wait()
    elementwise(range(E_BLOCKS - 3))
    own_x.wait()
    relay_step(0, 0)
    relay_step(0, 1)
    send_own(1)
    elementwise(range(E_BLOCKS - 3, E_BLOCKS))
    rest_step(0, 0)
    rest_step(0, 1)
    get_wd.wait()

    def grad_step(c, fresh):
        w = hidden // DY_CHUNKS
        pltpu.make_async_copy(mine_rows(c), mine_rows(c), dy_p.at[c]).wait()
        s = pl.ds(c * w, w)
        term = lax.dot_general(dy_all[:, s], wd[:, s], CONTRACT_COLS, preferred_element_type=F32)
        grad[...] = term if fresh else grad[...] + term

    def mine_rows(c):
        w = hidden // DY_CHUNKS
        return dy_all.at[pl.ds(0, 4 * ROWS), pl.ds(c * w, w)]

    far_step(0, 0)
    grad_step(0, True)
    far_step(0, 1)
    grad_step(2, False)
    grad_step(1, False)
    grad_step(3, False)
    n = tokens // E_BLOCKS
    for r in range(E_BLOCKS):
        s = pl.ds(r * n, n)
        g = grad[s, :]
        duu[s, :] = (g * act[s, :]).astype(BF16)
        dug[s, :] = (g * ugu[pl.ds(tokens + r * n, n), :].astype(F32) * slope[s, :]).astype(BF16)
    pltpu.make_async_copy(wgu, wgu, load_sem.at[2]).wait()

    def give_copy(h):
        s = pl.ds(h * DX_CHUNK, DX_CHUNK)
        return pltpu.make_async_remote_copy(
            src_ref=give.at[:, s], dst_ref=take.at[:, s], send_sem=give_sem.at[0], recv_sem=take_sem.at[h],
            device_id={'tp': other}, device_id_type=MESH)

    def combine(h):
        s = pl.ds(h * DX_CHUNK, DX_CHUNK)
        give_copy(h).wait_recv()
        for ref, device in ((own_out, me), (px_out, near_x), (py_out, near_y), (pd_out, far)):
            d = pl.ds(pl.multiple_of(lax.div(device, 2) * ROWS, ROWS), ROWS)
            ref[:, s] = (mine[d, s] + take[d, s].astype(F32)).astype(BF16)

    for h in range(n_dx):
        s = pl.ds(h * DX_CHUNK, DX_CHUNK)
        part[...] = (lax.dot_general(dug[...], wgu[s, :], CONTRACT_COLS, preferred_element_type=F32)
                     + lax.dot_general(duu[...], wgu[pl.ds(hidden + h * DX_CHUNK, DX_CHUNK), :], CONTRACT_COLS,
                                       preferred_element_type=F32))
        for j in range(4):
            d = pl.ds(j * ROWS, ROWS)
            give[d, s] = part[pl.ds(pl.multiple_of(j * 2 * ROWS + ROWS * (1 - core), ROWS), ROWS), :].astype(BF16)
            mine[d, s] = part[pl.ds(pl.multiple_of(j * 2 * ROWS + ROWS * core, ROWS), ROWS), :]
        give_copy(h).start()
        if h == 0:
            relay_step(1, 0)
        if h == 1:
            rest_step(1, 0)
            combine(0)
    for h in range(1, n_dx):
        combine(h)
    far_step(1, 0)
    pltpu.make_async_copy(give, give, give_sem.at[0]).wait()
    for a, buf in ((0, dy_all), (1, x_all)):
        everything = buf.at[pl.ds(0, 7 * ROWS), :]
        pltpu.make_async_copy(everything, everything, sent.at[a]).wait()
    from_partner = x_all.at[pl.ds(0, 4 * ROWS), :]
    pltpu.make_async_copy(from_partner, from_partner, x_p.at[0]).wait()


def gather_call(x, dy, wg, wu, wd, ug, uu):
    hidden, f = wg.shape
    tokens = ug.shape[0]
    n_dx = hidden // DX_CHUNK
    any_spec = pl.BlockSpec(memory_space=pl.ANY)
    x, dy, wg, wu, wd, ug, uu = [pltpu.with_memory_space_constraint(v, pltpu.HBM) for v in (x, dy, wg, wu, wd, ug, uu)]
    vmem, dma = pltpu.VMEM, pltpu.SemaphoreType.DMA
    full, act, row = vmem((tokens, hidden), BF16), vmem((tokens, f), BF16), vmem((ROWS, hidden), BF16)
    return pl.pallas_call(
        gather_kernel,
        out_shape=(full, full, act, act, act, row, row, row, row),
        in_specs=[any_spec] * 7,
        out_specs=[pl.BlockSpec(memory_space=vmem)] * 9,
        scratch_shapes=[
            vmem((2 * hidden, f), BF16), vmem((f, hidden), BF16), vmem((2 * tokens, f), BF16),
            vmem((tokens, f), F32), vmem((tokens, f), F32), vmem((tokens, f), F32), vmem((tokens, DX_CHUNK), F32),
            vmem((4 * ROWS, hidden), F32), vmem((4 * ROWS, hidden), BF16), vmem((4 * ROWS, hidden), BF16),
            dma((DY_CHUNKS,)), dma((DY_CHUNKS,)), dma((DY_CHUNKS,)), dma((DY_CHUNKS,)),
            dma((X_CHUNKS,)), dma((X_CHUNKS,)), dma((X_CHUNKS,)), dma((1,)),
            dma((2,)), dma((1,)), dma((n_dx,)), dma((2,)), dma((3,)),
        ],
        compiler_params=pltpu.CompilerParams(collective_id=0, has_side_effects=True, vmem_limit_bytes=48 * MIB),
        cost_estimate=pl.CostEstimate(flops=6 * tokens * hidden * f, bytes_accessed=24 * MIB, transcendentals=0),
        name='gather_and_input_grad',
    )(x, dy, wg, wu, wd, ug, uu)


def weight_kernel(x, dy, z, dug, duu, dwg, dwu, dwd):
    xb = x[...]
    dwg[...] = lax.dot_general(xb, dug[...], CONTRACT_ROWS, preferred_element_type=F32)
    dwu[...] = lax.dot_general(xb, duu[...], CONTRACT_ROWS, preferred_element_type=F32)
    dwd[...] = lax.dot_general(z[...], dy[...], CONTRACT_ROWS, preferred_element_type=F32)


def weight_call(x, dy, z, dug, duu, steps=12):
    tokens, hidden = x.shape
    f = z.shape[1]
    h = hidden // steps
    cols = pl.BlockSpec((tokens, h), lambda i: (0, i))
    whole = pl.BlockSpec((tokens, f), lambda i: (0, 0))
    tall = pl.BlockSpec((h, f), lambda i: (i, 0))
    wide = pl.BlockSpec((f, h), lambda i: (0, i))
    return pl.pallas_call(
        weight_kernel,
        grid=(steps,),
        in_specs=[cols, cols, whole, whole, whole],
        out_specs=[tall, tall, wide],
        out_shape=(jax.ShapeDtypeStruct((hidden, f), F32), jax.ShapeDtypeStruct((hidden, f), F32),
                   jax.ShapeDtypeStruct((f, hidden), F32)),
        compiler_params=pltpu.CompilerParams(vmem_limit_bytes=40 * MIB),
        cost_estimate=pl.CostEstimate(flops=6 * tokens * hidden * f, bytes_accessed=42 * MIB, transcendentals=0),
        name='weight_grads',
    )(x, dy, z, dug, duu)


def solution(mesh):
    n = mesh.shape['tp']

    def local_backward(x, wg, wu, wd, ug, uu, dy):
        x_all, dy_all, z, dug, duu, own, px, py, pd = gather_call(x, dy, wg, wu, wd, ug, uu)

        def swap(v, k):
            return lax.ppermute(v, 'tp', [(i, i ^ k) for i in range(n)])

        rx, ry, rd = swap(px, 2), swap(py, 4), swap(pd, 6)
        dwg, dwu, dwd = weight_call(x_all, dy_all, z, dug, duu)
        dx = (own.astype(F32) + rx.astype(F32) + ry.astype(F32) + rd.astype(F32)).astype(BF16)
        return dx, dwg, dwu, dwd

    tok_spec = P(('dp', 'tp'), None)
    col_spec = P(None, 'tp')
    act_spec = P('dp', 'tp')
    return jax.shard_map(local_backward, mesh=mesh,
                         in_specs=(tok_spec, col_spec, col_spec, P('tp', None), act_spec, act_spec, tok_spec),
                         out_specs=(tok_spec, act_spec, act_spec, tok_spec),
                         check_vma=False)
```
